32 devices in a mesh: ens: 2 (over core), ctx: 4 (over y, x), group: 4 (over z).
Axes of the slice: x: 2, y: 2, z: 4, core: 2. Of those that a mesh axis runs over, the one named last changes fastest.
Arguments:
- latents: bfloat16 [8, 1024, 512], P('ens', ('ctx', 'group')), parts along dimension 0, may hold values from -6 to 6
- rotary_rows: bfloat16 [8, 1024, 64], P('ens', ('ctx', 'group')), parts along dimension 0, may hold values from -6 to 6
- latent_gain: float32 [512], replicated, may hold values from 0.25 to 1.75
- key_up: bfloat16 [1024, 16, 128], P('ens', 'group'), parts along dimension 0, may hold values from -0.25 to 0.25
- value_up: bfloat16 [1024, 16, 128], P('ens', 'group'), parts along dimension 0, may hold values from -0.25 to 0.25
Outputs:
- stored_keys: bfloat16 [8, 16, 192, 1024], P(('ens', 'ctx'), 'group'), parts along dimension 0
- stored_values: bfloat16 [8, 1024, 16, 128], P(('ens', 'ctx'), None, 'group'), parts along dimension 0
The draws below stay inside these ranges and needn't reach their ends.
There are 2 independent parts, one for each index of `ens`. The reference program is written for one: setup_inputs(seed, part) draws one part's arguments, and reference() takes and returns one part's arrays. A program takes and returns all parts, laid end to end along the dimension named above; an argument that names none is the same for every part. Nothing has to cross between parts.
All inputs are finite; a program needn't handle non-finite values.
Results may differ from the reference program's by a relative error of at most 0.0049.
Values may be sent and summed in bfloat16 or wider, within the bound.
A program may use at most 64 MiB of HBM per device.

```python
import jax
import jax.numpy as jnp
from jax import lax

BATCH = 4
LENGTH = 1024
HEADS = 16
LATENT = 512
KEY_PART = 128
ROTARY = 64
VALUE_SIZE = 128


def levels(key, extent, split, low, top_value):
    loudness, own = 1.0, jax.random.fold_in(key, 6)
    for axis_at, shards_of in split:
        steps = jnp.exp(jax.random.uniform(jax.random.fold_in(own, axis_at), (shards_of,), jnp.float32, low / len(split), top_value / len(split)))
        loudness = loudness * jnp.repeat(steps, extent[axis_at] // shards_of).reshape([-1 if axis == axis_at else 1 for axis in range(len(extent))])
    return loudness


def gaussian(own_key, dims, width, reach, split=(), dtype=jnp.bfloat16):
    array = jax.random.normal(own_key, dims, jnp.float32) * width
    if len(split) > 0:
        array = levels(own_key, dims, split, -0.22, 0.18) * array
    return jnp.clip(array, min=-reach, max=reach).astype(dtype)


def setup_inputs(seed: int = 0, part: int = 0) -> dict:
    arg_keys = jax.random.split(jax.random.key(seed), 6)
    own_keys = jax.random.split(jax.random.fold_in(arg_keys[5], part), 6)
    latents = gaussian(own_keys[0], (BATCH, LENGTH, LATENT), 1.0, 6.0, ((1, 16),))
    rotary_rows = gaussian(own_keys[1], (BATCH, LENGTH, ROTARY), 1.0, 6.0, ((1, 16),))
    latent_gain = jnp.clip(1.0 + 0.15 * jax.random.normal(arg_keys[2], (LATENT,), jnp.float32), 0.25, 1.75)
    key_up = gaussian(own_keys[3], (LATENT, HEADS, KEY_PART), LATENT ** -0.5, 0.25, ((1, 4),))
    value_up = gaussian(own_keys[4], (LATENT, HEADS, VALUE_SIZE), LATENT ** -0.5, 0.25, ((1, 4),))
    return dict(latents=latents, rotary_rows=rotary_rows, latent_gain=latent_gain, key_up=key_up, value_up=value_up)


def root_norm(vectors, row_gain):
    return vectors * lax.rsqrt(lax.optimization_barrier(jnp.mean(vectors * vectors, axis=-1, keepdims=True)) + 1e-06) * row_gain

def reference(latents, rotary_rows, latent_gain, key_up, value_up):
    rows_ready = root_norm(latents.astype(jnp.float32), latent_gain).astype(jnp.bfloat16)
    rows_ready = lax.optimization_barrier(rows_ready)

    def expand_one(one):
        rows_one, rotary_one = one
        wide_keys = jnp.einsum('tr,rhk->thk', rows_one.astype(jnp.float32), key_up.astype(jnp.float32)).astype(jnp.bfloat16)
        shared = jnp.broadcast_to(rotary_one[:, None], (LENGTH, HEADS, ROTARY))
        wide_values = jnp.einsum('tr,rhk->thk', rows_one.astype(jnp.float32), value_up.astype(jnp.float32)).astype(jnp.bfloat16)
        return (jnp.concatenate([wide_keys, shared], axis=-1), wide_values)
    stored_keys, stored_values = lax.map(expand_one, (rows_ready, rotary_rows))
    stored_keys = jnp.transpose(stored_keys, (0, 2, 3, 1))
    return (stored_keys, stored_values)
```

```python
import functools

import jax
import jax.numpy as jnp
from jax import lax
from jax.experimental import pallas as pl
from jax.experimental.pallas import tpu as pltpu
from jax.sharding import PartitionSpec as P

MESH = pl.DeviceIdType.MESH
UNIT = 128


def partner(me, step, count):
    if count & (count - 1):
        return lax.rem(me + step, count)
    total, bit = 0, 1
    while bit < count:
        total = total + bit * lax.rem(me // bit + step // bit, 2)
        bit *= 2
    return total


def kernel(
    seqs, planes, heads,
    lat, rot, gain_in, key_up, value_up, keys, values,
    stage, raw, rot_stage, rot_pack, rot_raw, key_stage, value_stage,
    wide, key_w, value_w, mixed, gain,
    local_sem, got, got_rot, up, up_rot, down, down_rot, side, side_rot,
):
    c, g = lax.axis_index("ctx"), lax.axis_index("group")
    blk, latent = raw.shape[2], raw.shape[3]
    rotary = rot_stage.shape[2]
    half = blk // 2
    per_unit = UNIT // blk
    key_part = key_w.shape[0] // heads

    loads = [
        pltpu.make_async_copy(lat, stage, local_sem.at[0]),
        pltpu.make_async_copy(lat.at[c], raw.at[c, g], local_sem.at[1]),
        pltpu.make_async_copy(rot, rot_stage, local_sem.at[2]),
        pltpu.make_async_copy(key_up, key_stage, local_sem.at[3]),
        pltpu.make_async_copy(value_up, value_stage, local_sem.at[4]),
        pltpu.make_async_copy(gain_in, gain, local_sem.at[5]),
    ]
    for load in loads:
        load.start()

    barrier = pltpu.get_barrier_semaphore()

    @pl.loop(1, seqs)
    def _(b):
        pl.semaphore_signal(
            barrier, inc=1, device_id={"ctx": partner(c, b, seqs)}, device_id_type=MESH
        )

    @pl.when(g > 0)
    def _():
        pl.semaphore_signal(barrier, inc=1, device_id={"group": g - 1}, device_id_type=MESH)

    @pl.when(g < planes - 1)
    def _():
        pl.semaphore_signal(barrier, inc=1, device_id={"group": g + 1}, device_id_type=MESH)

    loads[2].wait()

    def pack(s):
        block = rot_stage[s].astype(jnp.float32)
        return jnp.concatenate([block[:half], block[half:]], axis=1).astype(jnp.bfloat16)

    @pl.loop(0, seqs)
    def _(s):
        rot_pack[s] = pack(s)

    rot_raw[c, g] = pack(c)
    loads[0].wait()
    loads[1].wait()
    peers = seqs - 1 + jnp.minimum(g, 1) + jnp.minimum(planes - 1 - g, 1)
    pl.semaphore_wait(barrier, peers)

    def along(p, q, buffer, out_sem, in_sem, to):
        return pltpu.make_async_remote_copy(
            src_ref=buffer.at[q, p], dst_ref=buffer.at[q, p],
            send_sem=out_sem.at[p, q], recv_sem=in_sem.at[p, q],
            device_id={"group": to}, device_id_type=MESH,
        )

    def upward(p, q):
        return along(p, q, raw, up, got, g + 1), along(p, q, rot_raw, up_rot, got_rot, g + 1)

    def downward(p, q):
        return (
            along(p, q, raw, down, got, g - 1),
            along(p, q, rot_raw, down_rot, got_rot, g - 1),
        )

    def across(s, source, buffer, out_sem, in_sem):
        return pltpu.make_async_remote_copy(
            src_ref=source.at[s], dst_ref=buffer.at[c, g],
            send_sem=out_sem.at[s], recv_sem=in_sem.at[g, c],
            device_id={"ctx": s}, device_id_type=MESH,
        )

    def sideways(s):
        return (
            across(s, stage, raw, side, got),
            across(s, rot_pack, rot_raw, side_rot, got_rot),
        )

    def send_up(p, q):
        @pl.when(g < planes - 1)
        def _():
            for copy in upward(p, q):
                copy.start()

    def send_down(p, q):
        @pl.when(g > 0)
        def _():
            for copy in downward(p, q):
                copy.start()

    def arrived(p, q):
        along(p, q, raw, up, got, g).wait_recv()
        along(p, q, rot_raw, up_rot, got_rot, g).wait_recv()

    @pl.loop(1, seqs)
    def _(b):
        across(partner(c, b, seqs), stage, raw, side, got).start()

    send_up(g, c)
    send_down(g, c)

    @pl.loop(1, seqs)
    def _(b):
        across(partner(c, b, seqs), rot_pack, rot_raw, side_rot, got_rot).start()

    loads[3].wait()
    wide[...] = key_stage[...].astype(jnp.float32)
    for h in range(heads):
        key_w[h * key_part : (h + 1) * key_part, :] = (
            wide[pl.ds(h, latent, stride=heads), :].T.astype(jnp.bfloat16)
        )
    loads[4].wait()
    loads[5].wait()
    wide[...] = value_stage[...].astype(jnp.float32)
    size = value_w.shape[1] // heads
    for h in range(heads):
        value_w[:, h * size : (h + 1) * size] = (
            wide[pl.ds(h, latent, stride=heads), :].astype(jnp.bfloat16)
        )

    def expand(q, u):
        first = u * per_unit
        x = raw[q, pl.ds(first, per_unit)].astype(jnp.float32).reshape(UNIT, latent)
        mean = jnp.mean(x * x, axis=-1, keepdims=True)
        rows = (x * lax.rsqrt(mean + 1e-06) * gain[...]).astype(jnp.bfloat16)
        start = pl.multiple_of((q * planes + first) * blk, UNIT)
        wide_keys = lax.dot_general(
            key_w[...], rows, (((1,), (1,)), ((), ())), preferred_element_type=jnp.float32
        ).astype(jnp.bfloat16)
        pieces = []
        for j in range(per_unit):
            both = rot_raw[q, first + j].astype(jnp.float32)
            pieces += [both[:, :rotary], pltpu.roll(both, rotary, 1)[:, :rotary]]
        turned = jnp.concatenate(pieces, axis=0).T.astype(jnp.bfloat16)
        for h in range(heads):
            keys[h, :key_part, pl.ds(start, UNIT)] = wide_keys[h * key_part : (h + 1) * key_part]
            keys[h, key_part:, pl.ds(start, UNIT)] = turned
        wide_values = jnp.dot(rows, value_w[...], preferred_element_type=jnp.float32)
        for h in range(heads):
            mixed[pl.ds(h, UNIT, stride=heads), :] = wide_values[:, h * size : (h + 1) * size]
        at = pl.multiple_of(start * heads, UNIT * heads)
        values[pl.ds(at, UNIT * heads), :] = mixed[...].astype(jnp.bfloat16)

    @pl.loop(1, seqs)
    def _(b):
        q = partner(c, b, seqs)
        arrived(g, q)
        send_up(g, q)
        send_down(g, q)

    @pl.loop(0, planes - 1)
    def _(r):
        @pl.loop(0, seqs)
        def _(b):
            q = partner(c, b, seqs)
            below, above = g - 1 - r, g + 1 + r

            @pl.when(below >= 0)
            def _():
                arrived(below, q)
                send_up(below, q)

            @pl.when(above < planes)
            def _():
                arrived(above, q)
                send_down(above, q)

            @pl.loop(0, planes // per_unit)
            def _(u):
                far = jnp.maximum(g - u * per_unit, (u + 1) * per_unit - 1 - g)

                @pl.when(far == r + 1)
                def _():
                    expand(q, u)

    @pl.loop(1, seqs)
    def _(b):
        for copy in sideways(partner(c, b, seqs)):
            copy.wait_send()

    @pl.loop(0, seqs)
    def _(q):
        @pl.loop(0, planes)
        def _(p):
            @pl.when((p <= g) & (g < planes - 1))
            def _():
                for copy in upward(p, q):
                    copy.wait_send()

            @pl.when((p >= g) & (g > 0))
            def _():
                for copy in downward(p, q):
                    copy.wait_send()


def per_device(latents, rotary_rows, latent_gain, key_up, value_up):
    seqs, planes = lax.axis_size("ctx"), lax.axis_size("group")
    _, blk, latent = latents.shape
    rotary = rotary_rows.shape[2]
    heads, key_part = key_up.shape[1:]
    size = value_up.shape[2]
    length = seqs * planes * blk
    bf16 = jnp.bfloat16
    dma = pltpu.SemaphoreType.DMA
    sent = (planes, seqs)
    in_hbm = functools.partial(pltpu.with_memory_space_constraint, memory_space=pltpu.HBM)
    anywhere = pl.BlockSpec(memory_space=pltpu.HBM)
    inside = pl.BlockSpec(memory_space=pltpu.VMEM)
    keys, values = pl.pallas_call(
        functools.partial(kernel, seqs, planes, heads),
        out_shape=(
            pltpu.VMEM((heads, key_part + rotary, length), bf16),
            pltpu.VMEM((length * heads, size), bf16),
        ),
        in_specs=[anywhere] * 5,
        out_specs=(inside, inside),
        scratch_shapes=[
            pltpu.VMEM((seqs, blk, latent), bf16),
            pltpu.VMEM((seqs, planes, blk, latent), bf16),
            pltpu.VMEM((seqs, blk, rotary), bf16),
            pltpu.VMEM((seqs, blk // 2, 2 * rotary), bf16),
            pltpu.VMEM((seqs, planes, blk // 2, 2 * rotary), bf16),
            pltpu.VMEM((latent * heads, key_part), bf16),
            pltpu.VMEM((latent * heads, size), bf16),
            pltpu.VMEM((latent * heads, size), jnp.float32),
            pltpu.VMEM((heads * key_part, latent), bf16),
            pltpu.VMEM((latent, heads * size), bf16),
            pltpu.VMEM((UNIT * heads, size), jnp.float32),
            pltpu.VMEM((1, latent), jnp.float32),
            dma((6,)),
            dma(sent), dma(sent), dma(sent), dma(sent), dma(sent), dma(sent),
            dma((seqs,)), dma((seqs,)),
        ],
        compiler_params=pltpu.CompilerParams(
            collective_id=0, has_side_effects=True, vmem_limit_bytes=32 * 1024 * 1024
        ),
    )(
        in_hbm(latents),
        in_hbm(rotary_rows),
        in_hbm(latent_gain.reshape(1, latent)),
        in_hbm(key_up.reshape(latent * heads, key_part)),
        in_hbm(value_up.reshape(latent * heads, size)),
    )
    return keys[None], values.reshape(1, length, heads, size)


def solution(mesh):
    in_specs = (
        P("ens", ("ctx", "group"), None),
        P("ens", ("ctx", "group"), None),
        P(),
        P("ens", "group", None),
        P("ens", "group", None),
    )
    out_specs = (P(("ens", "ctx"), "group", None, None), P(("ens", "ctx"), None, "group", None))
    return jax.shard_map(
        per_device, mesh=mesh, in_specs=in_specs, out_specs=out_specs, check_vma=False
    )
```

```python
import functools

import jax
import jax.numpy as jnp
from jax import lax
from jax.experimental import pallas as pl
from jax.experimental.pallas import tpu as pltpu
from jax.sharding import PartitionSpec as P

MESH = pl.DeviceIdType.MESH
LANES = 128


def partner(me, step, count):
    if count & (count - 1):
        return lax.rem(me + step, count)
    total, bit = 0, 1
    while bit < count:
        total = total + bit * lax.rem(me // bit + step // bit, 2)
        bit *= 2
    return total


def kernel(
    seqs, planes, heads, rotary,
    lat, rot, gain_in, key_up, value_up, keys, values,
    stage, raw, mid, rot_stage, key_stage, value_stage,
    wide, key_w, value_w, mixed, gain,
    lat_sem, local_sem, got, mid_got, own_up, own_down, side, mid_side, up, down,
):
    c, g = lax.axis_index("ctx"), lax.axis_index("group")
    blk, latent = lat.shape[1:]
    slabs = latent // LANES
    tail = slabs * blk
    half = blk // 2
    per_unit = LANES // blk
    key_part = key_w.shape[0] // heads
    size = value_w.shape[1] // heads

    lat_loads = [
        pltpu.make_async_copy(
            lat.at[:, :, pl.ds(k * LANES, LANES)],
            stage.at[:, pl.ds(k * blk, blk), :],
            lat_sem.at[k],
        )
        for k in range(slabs)
    ]
    loads = [
        pltpu.make_async_copy(rot, rot_stage, local_sem.at[0]),
        pltpu.make_async_copy(key_up, key_stage, local_sem.at[1]),
        pltpu.make_async_copy(value_up, value_stage, local_sem.at[2]),
        pltpu.make_async_copy(gain_in, gain, local_sem.at[3]),
    ]
    loads[0].start()
    for load in lat_loads + loads[1:]:
        load.start()

    barrier = pltpu.get_barrier_semaphore()

    @pl.loop(1, seqs)
    def _(b):
        pl.semaphore_signal(
            barrier, inc=1, device_id={"ctx": partner(c, b, seqs)}, device_id_type=MESH
        )

    @pl.when(g > 0)
    def _():
        pl.semaphore_signal(barrier, inc=1, device_id={"group": g - 1}, device_id_type=MESH)

    @pl.when(g < planes - 1)
    def _():
        pl.semaphore_signal(barrier, inc=1, device_id={"group": g + 1}, device_id_type=MESH)

    loads[0].wait()

    @pl.loop(0, seqs)
    def _(s):
        block = rot_stage[s].astype(jnp.float32)
        both = jnp.concatenate([block[:half], block[half:]], axis=1)
        stage[s, pl.ds(tail, half), :] = both.astype(jnp.bfloat16)

    for load in lat_loads:
        load.wait()
    peers = seqs - 1 + jnp.minimum(g, 1) + jnp.minimum(planes - 1 - g, 1)
    pl.semaphore_wait(barrier, peers)

    def remote(src, dst, out_sem, in_sem, to):
        return pltpu.make_async_remote_copy(
            src_ref=src, dst_ref=dst, send_sem=out_sem, recv_sem=in_sem,
            device_id=to, device_id_type=MESH,
        )

    def own_out(s, way, out_sem, to):
        return remote(
            stage.at[s], mid.at[way, s], out_sem.at[s], mid_got.at[way, s], {"group": to}
        )

    def own_along(out_sem, to):
        return remote(stage.at[c], raw.at[c, g], out_sem.at[c], got.at[g, c], {"group": to})

    def own_side(s):
        return remote(stage.at[s], raw.at[c, g], side.at[s], got.at[g, c], {"ctx": s})

    def scatter(way, s, p):
        return remote(
            mid.at[way, s], raw.at[c, p], mid_side.at[way, s], got.at[p, c], {"ctx": s}
        )

    def relay(p, q, out_sem, to):
        return remote(
            raw.at[q, p], raw.at[q, p], out_sem.at[p, q], got.at[p, q], {"group": to}
        )

    def arrived(p, q):
        relay(p, q, up, g).wait_recv()

    def relay_up(p, q):
        @pl.when(g < planes - 1)
        def _():
            relay(p, q, up, g + 1).start()

    def relay_down(p, q):
        @pl.when(g > 0)
        def _():
            relay(p, q, down, g - 1).start()

    def other(i):
        return partner(c, jnp.where(i == 1, seqs - 1, i - 1), seqs)

    @pl.loop(1, seqs)
    def _(i):
        s = other(i)

        @pl.when(g < planes - 1)
        def _():
            own_out(s, 0, own_up, g + 1).start()

        @pl.when(g > 0)
        def _():
            own_out(s, 1, own_down, g - 1).start()

        @pl.when(i == 1)
        def _():
            @pl.when(g < planes - 1)
            def _():
                own_along(own_up, g + 1).start()

            @pl.when(g > 0)
            def _():
                own_along(own_down, g - 1).start()

    @pl.loop(1, seqs)
    def _(i):
        own_side(partner(c, i, seqs)).start()

    raw[c, g] = stage[c]
    loads[1].wait()
    wide[...] = key_stage[...].astype(jnp.float32)
    for h in range(heads):
        key_w[h * key_part : (h + 1) * key_part, :] = (
            wide[pl.ds(h, latent, stride=heads), :].T.astype(jnp.bfloat16)
        )

    @pl.loop(1, seqs)
    def _(i):
        s = other(i)

        @pl.when(g > 0)
        def _():
            own_out(s, 0, own_up, g).wait_recv()
            scatter(0, s, g - 1).start()

        @pl.when(g < planes - 1)
        def _():
            own_out(s, 1, own_down, g).wait_recv()
            scatter(1, s, g + 1).start()

        @pl.when(i == 1)
        def _():
            @pl.when(g > 0)
            def _():
                arrived(g - 1, c)
                relay_up(g - 1, c)

            @pl.when(g < planes - 1)
            def _():
                arrived(g + 1, c)
                relay_down(g + 1, c)

    loads[2].wait()
    loads[3].wait()
    wide[...] = value_stage[...].astype(jnp.float32)
    for h in range(heads):
        value_w[:, h * size : (h + 1) * size] = (
            wide[pl.ds(h, latent, stride=heads), :].astype(jnp.bfloat16)
        )

    def expand(q, u):
        first = u * per_unit
        x = jnp.concatenate(
            [
                raw[q, pl.ds(first, per_unit), k * blk : (k + 1) * blk, :]
                .astype(jnp.float32)
                .reshape(LANES, LANES)
                for k in range(slabs)
            ],
            axis=1,
        )
        mean = jnp.mean(x * x, axis=-1, keepdims=True)
        rows = (x * lax.rsqrt(mean + 1e-06) * gain[...]).astype(jnp.bfloat16)
        start = pl.multiple_of((q * planes + first) * blk, LANES)
        wide_keys = lax.dot_general(
            key_w[...], rows, (((1,), (1,)), ((), ())), preferred_element_type=jnp.float32
        ).astype(jnp.bfloat16)
        pieces = []
        for j in range(per_unit):
            both = raw[q, first + j, tail:, :].astype(jnp.float32)
            pieces += [both[:, :rotary], pltpu.roll(both, rotary, 1)[:, :rotary]]
        turned = jnp.concatenate(pieces, axis=0).T.astype(jnp.bfloat16)
        for h in range(heads):
            keys[h, :key_part, pl.ds(start, LANES)] = wide_keys[h * key_part : (h + 1) * key_part]
            keys[h, key_part:, pl.ds(start, LANES)] = turned
        wide_values = jnp.dot(rows, value_w[...], preferred_element_type=jnp.float32)
        for h in range(heads):
            mixed[pl.ds(h, LANES, stride=heads), :] = wide_values[:, h * size : (h + 1) * size]
        at = pl.multiple_of(start * heads, LANES * heads)
        values[pl.ds(at, LANES * heads), :] = mixed[...].astype(jnp.bfloat16)

    def settle(r, q):
        @pl.loop(0, planes // per_unit)
        def _(u):
            far = jnp.maximum(g - u * per_unit, (u + 1) * per_unit - 1 - g)

            @pl.when(far == r + 1)
            def _():
                expand(q, u)

    @pl.loop(1, seqs)
    def _(i):
        q = other(i)

        @pl.when(g > 0)
        def _():
            arrived(g - 1, q)
            relay_up(g - 1, q)

        @pl.when(g < planes - 1)
        def _():
            arrived(g + 1, q)
            relay_down(g + 1, q)

    @pl.loop(1, seqs)
    def _(i):
        arrived(g, other(i))

    @pl.loop(0, planes - 1)
    def _(r):
        @pl.loop(0, seqs)
        def _(i):
            q = jnp.where(i == 0, c, other(i))
            below, above = g - 1 - r, g + 1 + r

            @pl.when((r > 0) & (below >= 0))
            def _():
                arrived(below, q)
                relay_up(below, q)

            @pl.when((r > 0) & (above < planes))
            def _():
                arrived(above, q)
                relay_down(above, q)

            settle(r, q)

    @pl.loop(0, seqs)
    def _(s):
        @pl.when(g < planes - 1)
        def _():
            own_out(s, 0, own_up, g).wait_send()

        @pl.when(g > 0)
        def _():
            own_out(s, 1, own_down, g).wait_send()

        @pl.when(s != c)
        def _():
            own_side(s).wait_send()

            @pl.when(g > 0)
            def _():
                scatter(0, s, g).wait_send()

            @pl.when(g < planes - 1)
            def _():
                scatter(1, s, g).wait_send()

        @pl.loop(0, planes)
        def _(p):
            @pl.when((p < g) & (g < planes - 1))
            def _():
                relay(p, s, up, g).wait_send()

            @pl.when((p > g) & (g > 0))
            def _():
                relay(p, s, down, g).wait_send()


def per_device(latents, rotary_rows, latent_gain, key_up, value_up):
    seqs, planes = lax.axis_size("ctx"), lax.axis_size("group")
    _, blk, latent = latents.shape
    rotary = rotary_rows.shape[2]
    heads, key_part = key_up.shape[1:]
    size = value_up.shape[2]
    length = seqs * planes * blk
    packed = (blk * (latent + rotary) // LANES, LANES)
    bf16 = jnp.bfloat16
    dma = pltpu.SemaphoreType.DMA
    in_hbm = functools.partial(pltpu.with_memory_space_constraint, memory_space=pltpu.HBM)
    outer = pl.BlockSpec(memory_space=pltpu.HBM)
    inside = pl.BlockSpec(memory_space=pltpu.VMEM)
    keys, values = pl.pallas_call(
        functools.partial(kernel, seqs, planes, heads, rotary),
        out_shape=(
            pltpu.VMEM((heads, key_part + rotary, length), bf16),
            pltpu.VMEM((length * heads, size), bf16),
        ),
        in_specs=[outer] * 5,
        out_specs=(inside, inside),
        scratch_shapes=[
            pltpu.VMEM((seqs, *packed), bf16),
            pltpu.VMEM((seqs, planes, *packed), bf16),
            pltpu.VMEM((2, seqs, *packed), bf16),
            pltpu.VMEM((seqs, blk, rotary), bf16),
            pltpu.VMEM((latent * heads, key_part), bf16),
            pltpu.VMEM((latent * heads, size), bf16),
            pltpu.VMEM((latent * heads, size), jnp.float32),
            pltpu.VMEM((heads * key_part, latent), bf16),
            pltpu.VMEM((latent, heads * size), bf16),
            pltpu.VMEM((LANES * heads, size), jnp.float32),
            pltpu.VMEM((1, latent), jnp.float32),
            dma((latent // LANES,)),
            dma((4,)),
            dma((planes, seqs)),
            dma((2, seqs)),
            dma((seqs,)), dma((seqs,)), dma((seqs,)),
            dma((2, seqs)),
            dma((planes, seqs)), dma((planes, seqs)),
        ],
        compiler_params=pltpu.CompilerParams(
            collective_id=0, has_side_effects=True, vmem_limit_bytes=32 * 1024 * 1024
        ),
    )(
        in_hbm(latents),
        in_hbm(rotary_rows),
        in_hbm(latent_gain.reshape(1, latent)),
        in_hbm(key_up.reshape(latent * heads, key_part)),
        in_hbm(value_up.reshape(latent * heads, size)),
    )
    return keys[None], values.reshape(1, length, heads, size)


def solution(mesh):
    in_specs = (
        P("ens", ("ctx", "group"), None),
        P("ens", ("ctx", "group"), None),
        P(),
        P("ens", "group", None),
        P("ens", "group", None),
    )
    out_specs = (P(("ens", "ctx"), "group", None, None), P(("ens", "ctx"), None, "group", None))
    return jax.shard_map(
        per_device, mesh=mesh, in_specs=in_specs, out_specs=out_specs, check_vma=False
    )
```

```python
import functools

import jax
import jax.numpy as jnp
from jax import lax
from jax.experimental import pallas as pl
from jax.experimental.pallas import tpu as pltpu
from jax.sharding import PartitionSpec as P

MESH = pl.DeviceIdType.MESH
LANES = 128


def partner(me, step, count):
    if count & (count - 1):
        return lax.rem(me + step, count)
    total, bit = 0, 1
    while bit < count:
        total = total + bit * lax.rem(me // bit + step // bit, 2)
        bit *= 2
    return total


def kernel(
    seqs, planes, heads, rotary,
    lat, rot, gain_in, key_up, value_up, keys, values,
    stage, raw, mid, rot_stage, key_stage, value_stage,
    wide, key_w, value_w, mixed, gain,
    lat_sem, local_sem, got, mid_got, own_up, own_down, side, mid_side, up, down,
):
    c, g = lax.axis_index("ctx"), lax.axis_index("group")
    blk, latent = lat.shape[1:]
    slabs = latent // LANES
    tail = slabs * blk
    half = blk // 2
    per_unit = LANES // blk
    key_part = key_w.shape[0] // heads
    size = value_w.shape[1] // heads

    lat_loads = [
        pltpu.make_async_copy(
            lat.at[:, :, pl.ds(k * LANES, LANES)],
            stage.at[:, pl.ds(k * blk, blk), :],
            lat_sem.at[k],
        )
        for k in range(slabs)
    ]
    loads = [
        pltpu.make_async_copy(rot, rot_stage, local_sem.at[0]),
        pltpu.make_async_copy(key_up, key_stage, local_sem.at[1]),
        pltpu.make_async_copy(value_up, value_stage, local_sem.at[2]),
        pltpu.make_async_copy(gain_in, gain, local_sem.at[3]),
    ]
    loads[0].start()
    for load in lat_loads + loads[1:]:
        load.start()

    barrier = pltpu.get_barrier_semaphore()

    @pl.loop(1, seqs)
    def _(b):
        pl.semaphore_signal(
            barrier, inc=1, device_id={"ctx": partner(c, b, seqs)}, device_id_type=MESH
        )

    @pl.when(g > 0)
    def _():
        pl.semaphore_signal(barrier, inc=1, device_id={"group": g - 1}, device_id_type=MESH)

    @pl.when(g < planes - 1)
    def _():
        pl.semaphore_signal(barrier, inc=1, device_id={"group": g + 1}, device_id_type=MESH)

    loads[0].wait()

    @pl.loop(0, seqs)
    def _(s):
        block = rot_stage[s].astype(jnp.float32)
        both = jnp.concatenate([block[:half], block[half:]], axis=1)
        stage[s, pl.ds(tail, half), :] = both.astype(jnp.bfloat16)

    for load in lat_loads:
        load.wait()
    peers = seqs - 1 + jnp.minimum(g, 1) + jnp.minimum(planes - 1 - g, 1)
    pl.semaphore_wait(barrier, peers)

    def remote(src, dst, out_sem, in_sem, to):
        return pltpu.make_async_remote_copy(
            src_ref=src, dst_ref=dst, send_sem=out_sem, recv_sem=in_sem,
            device_id=to, device_id_type=MESH,
        )

    def own_out(s, way, out_sem, to):
        return remote(
            stage.at[s], mid.at[way, s], out_sem.at[s], mid_got.at[way, s], {"group": to}
        )

    def own_along(out_sem, to):
        return remote(stage.at[c], raw.at[c, g], out_sem.at[c], got.at[g, c], {"group": to})

    def own_side(s):
        return remote(stage.at[s], raw.at[c, g], side.at[s], got.at[g, c], {"ctx": s})

    def scatter(way, s, p):
        return remote(
            mid.at[way, s], raw.at[c, p], mid_side.at[way, s], got.at[p, c], {"ctx": s}
        )

    def relay(p, q, out_sem, to):
        return remote(
            raw.at[q, p], raw.at[q, p], out_sem.at[p, q], got.at[p, q], {"group": to}
        )

    def arrived(p, q):
        relay(p, q, up, g).wait_recv()

    def relay_up(p, q):
        @pl.when(g < planes - 1)
        def _():
            relay(p, q, up, g + 1).start()

    def relay_down(p, q):
        @pl.when(g > 0)
        def _():
            relay(p, q, down, g - 1).start()

    def other(i):
        return partner(c, jnp.where(i == 1, seqs - 1, i - 1), seqs)

    @pl.loop(1, seqs)
    def _(i):
        s = other(i)

        @pl.when(g < planes - 1)
        def _():
            own_out(s, 0, own_up, g + 1).start()

        @pl.when(g > 0)
        def _():
            own_out(s, 1, own_down, g - 1).start()

        @pl.when(i == 1)
        def _():
            @pl.when(g < planes - 1)
            def _():
                own_along(own_up, g + 1).start()

            @pl.when(g > 0)
            def _():
                own_along(own_down, g - 1).start()

    @pl.loop(1, seqs)
    def _(i):
        own_side(partner(c, i, seqs)).start()

    raw[c, g] = stage[c]
    loads[1].wait()
    wide[...] = key_stage[...].astype(jnp.float32)
    for h in range(heads):
        key_w[h * key_part : (h + 1) * key_part, :] = (
            wide[pl.ds(h, latent, stride=heads), :].T.astype(jnp.bfloat16)
        )

    loads[2].wait()
    loads[3].wait()
    wide[...] = value_stage[...].astype(jnp.float32)
    for h in range(heads):
        value_w[:, h * size : (h + 1) * size] = (
            wide[pl.ds(h, latent, stride=heads), :].astype(jnp.bfloat16)
        )

    @pl.loop(1, seqs)
    def _(i):
        s = other(i)

        @pl.when(g > 0)
        def _():
            own_out(s, 0, own_up, g).wait_recv()
            scatter(0, s, g - 1).start()

        @pl.when(g < planes - 1)
        def _():
            own_out(s, 1, own_down, g).wait_recv()
            scatter(1, s, g + 1).start()

        @pl.when(i == 1)
        def _():
            @pl.when(g > 0)
            def _():
                arrived(g - 1, c)
                relay_up(g - 1, c)

            @pl.when(g < planes - 1)
            def _():
                arrived(g + 1, c)
                relay_down(g + 1, c)

    def expand(q, u):
        first = u * per_unit
        x = jnp.concatenate(
            [
                raw[q, pl.ds(first, per_unit), k * blk : (k + 1) * blk, :]
                .astype(jnp.float32)
                .reshape(LANES, LANES)
                for k in range(slabs)
            ],
            axis=1,
        )
        mean = jnp.mean(x * x, axis=-1, keepdims=True)
        rows = (x * lax.rsqrt(mean + 1e-06) * gain[...]).astype(jnp.bfloat16)
        start = pl.multiple_of((q * planes + first) * blk, LANES)
        wide_keys = lax.dot_general(
            key_w[...], rows, (((1,), (1,)), ((), ())), preferred_element_type=jnp.float32
        ).astype(jnp.bfloat16)
        pieces = []
        for j in range(per_unit):
            both = raw[q, first + j, tail:, :].astype(jnp.float32)
            pieces += [both[:, :rotary], pltpu.roll(both, rotary, 1)[:, :rotary]]
        turned = jnp.concatenate(pieces, axis=0).T.astype(jnp.bfloat16)
        for h in range(heads):
            keys[h, :key_part, pl.ds(start, LANES)] = wide_keys[h * key_part : (h + 1) * key_part]
            keys[h, key_part:, pl.ds(start, LANES)] = turned
        wide_values = jnp.dot(rows, value_w[...], preferred_element_type=jnp.float32)
        for h in range(heads):
            mixed[pl.ds(h, LANES, stride=heads), :] = wide_values[:, h * size : (h + 1) * size]
        at = pl.multiple_of(start * heads, LANES * heads)
        values[pl.ds(at, LANES * heads), :] = mixed[...].astype(jnp.bfloat16)

    def settle(q, low, high):
        @pl.loop(0, planes // per_unit)
        def _(u):
            far = jnp.maximum(g - u * per_unit, (u + 1) * per_unit - 1 - g)
            far = jnp.maximum(far, 1)

            @pl.when((far >= low) & (far <= high))
            def _():
                expand(q, u)

    @pl.loop(1, seqs)
    def _(i):
        q = other(i)

        @pl.when(g > 0)
        def _():
            arrived(g - 1, q)
            relay_up(g - 1, q)

        @pl.when(g < planes - 1)
        def _():
            arrived(g + 1, q)
            relay_down(g + 1, q)

    @pl.loop(1, seqs)
    def _(i):
        arrived(g, other(i))

    @pl.loop(1, max(planes - 1, 2))
    def _(r):
        @pl.loop(0, seqs)
        def _(i):
            q = jnp.where(i == 0, c, other(i))
            below, above = g - 1 - r, g + 1 + r

            @pl.when(below >= 0)
            def _():
                arrived(below, q)
                relay_up(below, q)

            @pl.when(above < planes)
            def _():
                arrived(above, q)
                relay_down(above, q)

            settle(q, r, jnp.where(r == planes - 2, r + 1, r))

    @pl.loop(0, seqs)
    def _(s):
        @pl.when(g < planes - 1)
        def _():
            own_out(s, 0, own_up, g).wait_send()

        @pl.when(g > 0)
        def _():
            own_out(s, 1, own_down, g).wait_send()

        @pl.when(s != c)
        def _():
            own_side(s).wait_send()

            @pl.when(g > 0)
            def _():
                scatter(0, s, g).wait_send()

            @pl.when(g < planes - 1)
            def _():
                scatter(1, s, g).wait_send()

        @pl.loop(0, planes)
        def _(p):
            @pl.when((p < g) & (g < planes - 1))
            def _():
                relay(p, s, up, g).wait_send()

            @pl.when((p > g) & (g > 0))
            def _():
                relay(p, s, down, g).wait_send()


def store(keys, values, keys_out, values_out, sems):
    pieces = sems.shape[0] // 2
    rows = values.shape[0] // pieces
    heads = keys.shape[0] // pieces
    copies = []
    for i in range(pieces):
        part = pl.ds(i * heads, heads)
        copies.append(pltpu.make_async_copy(keys.at[part], keys_out.at[part], sems.at[2 * i]))
        part = pl.ds(i * rows, rows)
        copies.append(
            pltpu.make_async_copy(values.at[part], values_out.at[part], sems.at[2 * i + 1])
        )
    for copy in copies:
        copy.start()
    for copy in copies:
        copy.wait()


def per_device(latents, rotary_rows, latent_gain, key_up, value_up):
    seqs, planes = lax.axis_size("ctx"), lax.axis_size("group")
    _, blk, latent = latents.shape
    rotary = rotary_rows.shape[2]
    heads, key_part = key_up.shape[1:]
    size = value_up.shape[2]
    length = seqs * planes * blk
    packed = (blk * (latent + rotary) // LANES, LANES)
    bf16 = jnp.bfloat16
    dma = pltpu.SemaphoreType.DMA
    in_hbm = functools.partial(pltpu.with_memory_space_constraint, memory_space=pltpu.HBM)
    outer = pl.BlockSpec(memory_space=pltpu.HBM)
    inside = pl.BlockSpec(memory_space=pltpu.VMEM)
    keys, values = pl.pallas_call(
        functools.partial(kernel, seqs, planes, heads, rotary),
        out_shape=(
            pltpu.VMEM((heads, key_part + rotary, length), bf16),
            pltpu.VMEM((length * heads, size), bf16),
        ),
        in_specs=[outer] * 5,
        out_specs=(inside, inside),
        scratch_shapes=[
            pltpu.VMEM((seqs, *packed), bf16),
            pltpu.VMEM((seqs, planes, *packed), bf16),
            pltpu.VMEM((2, seqs, *packed), bf16),
            pltpu.VMEM((seqs, blk, rotary), bf16),
            pltpu.VMEM((latent * heads, key_part), bf16),
            pltpu.VMEM((latent * heads, size), bf16),
            pltpu.VMEM((latent * heads, size), jnp.float32),
            pltpu.VMEM((heads * key_part, latent), bf16),
            pltpu.VMEM((latent, heads * size), bf16),
            pltpu.VMEM((LANES * heads, size), jnp.float32),
            pltpu.VMEM((1, latent), jnp.float32),
            dma((latent // LANES,)),
            dma((4,)),
            dma((planes, seqs)),
            dma((2, seqs)),
            dma((seqs,)), dma((seqs,)), dma((seqs,)),
            dma((2, seqs)),
            dma((planes, seqs)), dma((planes, seqs)),
        ],
        compiler_params=pltpu.CompilerParams(
            collective_id=0, has_side_effects=True, vmem_limit_bytes=32 * 1024 * 1024
        ),
    )(
        in_hbm(latents),
        in_hbm(rotary_rows),
        in_hbm(latent_gain.reshape(1, latent)),
        in_hbm(key_up.reshape(latent * heads, key_part)),
        in_hbm(value_up.reshape(latent * heads, size)),
    )
    keys, values = pl.pallas_call(
        store,
        out_shape=(
            jax.ShapeDtypeStruct(keys.shape, bf16),
            jax.ShapeDtypeStruct(values.shape, bf16),
        ),
        in_specs=[inside, inside],
        out_specs=(outer, outer),
        scratch_shapes=[dma((2 * heads,))],
        compiler_params=pltpu.CompilerParams(vmem_limit_bytes=16 * 1024 * 1024),
    )(keys, values)
    return keys[None], values.reshape(1, length, heads, size)


def solution(mesh):
    in_specs = (
        P("ens", ("ctx", "group"), None),
        P("ens", ("ctx", "group"), None),
        P(),
        P("ens", "group", None),
        P("ens", "group", None),
    )
    out_specs = (P(("ens", "ctx"), "group", None, None), P(("ens", "ctx"), None, "group", None))
    return jax.shard_map(
        per_device, mesh=mesh, in_specs=in_specs, out_specs=out_specs, check_vma=False
    )
```

```python
import functools

import jax
import jax.numpy as jnp
from jax import lax
from jax.experimental import pallas as pl
from jax.experimental.pallas import tpu as pltpu
from jax.sharding import PartitionSpec as P

MESH = pl.DeviceIdType.MESH
LANES = 128


def partner(me, step, count):
    if count & (count - 1):
        return lax.rem(me + step, count)
    total, bit = 0, 1
    while bit < count:
        total = total + bit * lax.rem(me // bit + step // bit, 2)
        bit *= 2
    return total


def kernel(
    seqs, planes, heads, rotary,
    lat, rot, gain_in, key_up, value_up, keys, values,
    stage, raw, mid, rot_stage, key_stage, value_stage,
    wide, key_w, value_w, mixed, gain,
    lat_sem, local_sem, got, mid_got, own_up, own_down, side, mid_side, up, down,
):
    c, g = lax.axis_index("ctx"), lax.axis_index("group")
    blk, latent = lat.shape[1:]
    slabs = latent // LANES
    tail = slabs * blk
    half = blk // 2
    per_unit = LANES // blk
    key_part = key_w.shape[0] // heads
    size = value_w.shape[1] // heads

    lat_loads = [
        pltpu.make_async_copy(
            lat.at[:, :, pl.ds(k * LANES, LANES)],
            stage.at[:, pl.ds(k * blk, blk), :],
            lat_sem.at[k],
        )
        for k in range(slabs)
    ]
    loads = [
        pltpu.make_async_copy(rot, rot_stage, local_sem.at[0]),
        pltpu.make_async_copy(key_up, key_stage, local_sem.at[1]),
        pltpu.make_async_copy(value_up, value_stage, local_sem.at[2]),
        pltpu.make_async_copy(gain_in, gain, local_sem.at[3]),
    ]
    loads[0].start()
    for load in lat_loads + loads[1:]:
        load.start()

    barrier = pltpu.get_barrier_semaphore()

    @pl.loop(1, seqs)
    def _(b):
        pl.semaphore_signal(
            barrier, inc=1, device_id={"ctx": partner(c, b, seqs)}, device_id_type=MESH
        )

    @pl.when(g > 0)
    def _():
        pl.semaphore_signal(barrier, inc=1, device_id={"group": g - 1}, device_id_type=MESH)

    @pl.when(g < planes - 1)
    def _():
        pl.semaphore_signal(barrier, inc=1, device_id={"group": g + 1}, device_id_type=MESH)

    loads[0].wait()

    @pl.loop(0, seqs)
    def _(s):
        block = rot_stage[s].astype(jnp.float32)
        both = jnp.concatenate([block[:half], block[half:]], axis=1)
        stage[s, pl.ds(tail, half), :] = both.astype(jnp.bfloat16)

    for load in lat_loads:
        load.wait()
    peers = seqs - 1 + jnp.minimum(g, 1) + jnp.minimum(planes - 1 - g, 1)
    pl.semaphore_wait(barrier, peers)

    def remote(src, dst, out_sem, in_sem, to):
        return pltpu.make_async_remote_copy(
            src_ref=src, dst_ref=dst, send_sem=out_sem, recv_sem=in_sem,
            device_id=to, device_id_type=MESH,
        )

    def own_out(s, way, out_sem, to):
        return remote(
            stage.at[s], mid.at[way, s], out_sem.at[s], mid_got.at[way, s], {"group": to}
        )

    def own_along(out_sem, to):
        return remote(stage.at[c], raw.at[c, g], out_sem.at[c], got.at[g, c], {"group": to})

    def own_side(s):
        return remote(stage.at[s], raw.at[c, g], side.at[s], got.at[g, c], {"ctx": s})

    def scatter(way, s, p):
        return remote(
            mid.at[way, s], raw.at[c, p], mid_side.at[way, s], got.at[p, c], {"ctx": s}
        )

    def relay(p, q, out_sem, to):
        return remote(
            raw.at[q, p], raw.at[q, p], out_sem.at[p, q], got.at[p, q], {"group": to}
        )

    def arrived(p, q):
        relay(p, q, up, g).wait_recv()

    def relay_up(p, q):
        @pl.when(g < planes - 1)
        def _():
            relay(p, q, up, g + 1).start()

    def relay_down(p, q):
        @pl.when(g > 0)
        def _():
            relay(p, q, down, g - 1).start()

    def other(i):
        return partner(c, jnp.where(i == 1, seqs - 1, i - 1), seqs)

    @pl.loop(1, seqs)
    def _(i):
        s = other(i)

        @pl.when(g < planes - 1)
        def _():
            own_out(s, 0, own_up, g + 1).start()

        @pl.when(g > 0)
        def _():
            own_out(s, 1, own_down, g - 1).start()

        @pl.when(i == 1)
        def _():
            @pl.when(g < planes - 1)
            def _():
                own_along(own_up, g + 1).start()

            @pl.when(g > 0)
            def _():
                own_along(own_down, g - 1).start()

    @pl.loop(1, seqs)
    def _(i):
        own_side(partner(c, i, seqs)).start()

    raw[c, g] = stage[c]
    loads[1].wait()
    wide[...] = key_stage[...].astype(jnp.float32)
    for h in range(heads):
        key_w[h * key_part : (h + 1) * key_part, :] = (
            wide[pl.ds(h, latent, stride=heads), :].T.astype(jnp.bfloat16)
        )

    loads[2].wait()
    loads[3].wait()
    wide[...] = value_stage[...].astype(jnp.float32)
    for h in range(heads):
        value_w[:, h * size : (h + 1) * size] = (
            wide[pl.ds(h, latent, stride=heads), :].astype(jnp.bfloat16)
        )

    low = 2 * g < planes

    def near_first(from_below, from_above):
        pl.when(low)(from_above)
        from_below()
        pl.when(jnp.logical_not(low))(from_above)

    @pl.loop(1, seqs)
    def _(i):
        s = other(i)

        def spread_below():
            @pl.when(g > 0)
            def _():
                own_out(s, 0, own_up, g).wait_recv()
                scatter(0, s, g - 1).start()

        def spread_above():
            @pl.when(g < planes - 1)
            def _():
                own_out(s, 1, own_down, g).wait_recv()
                scatter(1, s, g + 1).start()

        near_first(spread_below, spread_above)

        def own_below():
            @pl.when(g > 0)
            def _():
                arrived(g - 1, c)
                relay_up(g - 1, c)

        def own_above():
            @pl.when(g < planes - 1)
            def _():
                arrived(g + 1, c)
                relay_down(g + 1, c)

        @pl.when(i == 1)
        def _():
            near_first(own_below, own_above)

    def expand(q, u):
        first = u * per_unit
        x = jnp.concatenate(
            [
                raw[q, pl.ds(first, per_unit), k * blk : (k + 1) * blk, :]
                .astype(jnp.float32)
                .reshape(LANES, LANES)
                for k in range(slabs)
            ],
            axis=1,
        )
        mean = jnp.mean(x * x, axis=-1, keepdims=True)
        rows = (x * lax.rsqrt(mean + 1e-06) * gain[...]).astype(jnp.bfloat16)
        start = pl.multiple_of((q * planes + first) * blk, LANES)
        wide_keys = lax.dot_general(
            key_w[...], rows, (((1,), (1,)), ((), ())), preferred_element_type=jnp.float32
        ).astype(jnp.bfloat16)
        pieces = []
        for j in range(per_unit):
            both = raw[q, first + j, tail:, :].astype(jnp.float32)
            pieces += [both[:, :rotary], pltpu.roll(both, rotary, 1)[:, :rotary]]
        turned = jnp.concatenate(pieces, axis=0).T.astype(jnp.bfloat16)
        for h in range(heads):
            keys[h, :key_part, pl.ds(start, LANES)] = wide_keys[h * key_part : (h + 1) * key_part]
            keys[h, key_part:, pl.ds(start, LANES)] = turned
        wide_values = jnp.dot(rows, value_w[...], preferred_element_type=jnp.float32)
        for h in range(heads):
            mixed[pl.ds(h, LANES, stride=heads), :] = wide_values[:, h * size : (h + 1) * size]
        at = pl.multiple_of(start * heads, LANES * heads)
        values[pl.ds(at, LANES * heads), :] = mixed[...].astype(jnp.bfloat16)

    def settle(q, low, high):
        @pl.loop(0, planes // per_unit)
        def _(u):
            far = jnp.maximum(g - u * per_unit, (u + 1) * per_unit - 1 - g)
            far = jnp.maximum(far, 1)

            @pl.when((far >= low) & (far <= high))
            def _():
                expand(q, u)

    @pl.loop(1, seqs)
    def _(i):
        q = other(i)

        def next_below():
            @pl.when(g > 0)
            def _():
                arrived(g - 1, q)
                relay_up(g - 1, q)

        def next_above():
            @pl.when(g < planes - 1)
            def _():
                arrived(g + 1, q)
                relay_down(g + 1, q)

        near_first(next_below, next_above)

    @pl.loop(1, seqs)
    def _(i):
        arrived(g, other(i))

    @pl.loop(1, max(planes - 1, 2))
    def _(r):
        @pl.loop(0, seqs)
        def _(i):
            q = jnp.where(i == 0, c, other(i))
            below, above = g - 1 - r, g + 1 + r

            @pl.when(below >= 0)
            def _():
                arrived(below, q)
                relay_up(below, q)

            @pl.when(above < planes)
            def _():
                arrived(above, q)
                relay_down(above, q)

            settle(q, r, jnp.where(r == planes - 2, r + 1, r))

    @pl.loop(0, seqs)
    def _(s):
        @pl.when(g < planes - 1)
        def _():
            own_out(s, 0, own_up, g).wait_send()

        @pl.when(g > 0)
        def _():
            own_out(s, 1, own_down, g).wait_send()

        @pl.when(s != c)
        def _():
            own_side(s).wait_send()

            @pl.when(g > 0)
            def _():
                scatter(0, s, g).wait_send()

            @pl.when(g < planes - 1)
            def _():
                scatter(1, s, g).wait_send()

        @pl.loop(0, planes)
        def _(p):
            @pl.when((p < g) & (g < planes - 1))
            def _():
                relay(p, s, up, g).wait_send()

            @pl.when((p > g) & (g > 0))
            def _():
                relay(p, s, down, g).wait_send()


def store(keys, values, keys_out, values_out, sems):
    pieces = sems.shape[0] // 2
    rows = values.shape[0] // pieces
    heads = keys.shape[0] // pieces
    copies = []
    for i in range(pieces):
        part = pl.ds(i * heads, heads)
        copies.append(pltpu.make_async_copy(keys.at[part], keys_out.at[part], sems.at[2 * i]))
        part = pl.ds(i * rows, rows)
        copies.append(
            pltpu.make_async_copy(values.at[part], values_out.at[part], sems.at[2 * i + 1])
        )
    for copy in copies:
        copy.start()
    for copy in copies:
        copy.wait()


def per_device(latents, rotary_rows, latent_gain, key_up, value_up):
    seqs, planes = lax.axis_size("ctx"), lax.axis_size("group")
    _, blk, latent = latents.shape
    rotary = rotary_rows.shape[2]
    heads, key_part = key_up.shape[1:]
    size = value_up.shape[2]
    length = seqs * planes * blk
    packed = (blk * (latent + rotary) // LANES, LANES)
    bf16 = jnp.bfloat16
    dma = pltpu.SemaphoreType.DMA
    in_hbm = functools.partial(pltpu.with_memory_space_constraint, memory_space=pltpu.HBM)
    outer = pl.BlockSpec(memory_space=pltpu.HBM)
    inside = pl.BlockSpec(memory_space=pltpu.VMEM)
    keys, values = pl.pallas_call(
        functools.partial(kernel, seqs, planes, heads, rotary),
        out_shape=(
            pltpu.VMEM((heads, key_part + rotary, length), bf16),
            pltpu.VMEM((length * heads, size), bf16),
        ),
        in_specs=[outer] * 5,
        out_specs=(inside, inside),
        scratch_shapes=[
            pltpu.VMEM((seqs, *packed), bf16),
            pltpu.VMEM((seqs, planes, *packed), bf16),
            pltpu.VMEM((2, seqs, *packed), bf16),
            pltpu.VMEM((seqs, blk, rotary), bf16),
            pltpu.VMEM((latent * heads, key_part), bf16),
            pltpu.VMEM((latent * heads, size), bf16),
            pltpu.VMEM((latent * heads, size), jnp.float32),
            pltpu.VMEM((heads * key_part, latent), bf16),
            pltpu.VMEM((latent, heads * size), bf16),
            pltpu.VMEM((LANES * heads, size), jnp.float32),
            pltpu.VMEM((1, latent), jnp.float32),
            dma((latent // LANES,)),
            dma((4,)),
            dma((planes, seqs)),
            dma((2, seqs)),
            dma((seqs,)), dma((seqs,)), dma((seqs,)),
            dma((2, seqs)),
            dma((planes, seqs)), dma((planes, seqs)),
        ],
        compiler_params=pltpu.CompilerParams(
            collective_id=0, has_side_effects=True, vmem_limit_bytes=32 * 1024 * 1024
        ),
    )(
        in_hbm(latents),
        in_hbm(rotary_rows),
        in_hbm(latent_gain.reshape(1, latent)),
        in_hbm(key_up.reshape(latent * heads, key_part)),
        in_hbm(value_up.reshape(latent * heads, size)),
    )
    keys, values = pl.pallas_call(
        store,
        out_shape=(
            jax.ShapeDtypeStruct(keys.shape, bf16),
            jax.ShapeDtypeStruct(values.shape, bf16),
        ),
        in_specs=[inside, inside],
        out_specs=(outer, outer),
        scratch_shapes=[dma((2 * heads,))],
        compiler_params=pltpu.CompilerParams(vmem_limit_bytes=16 * 1024 * 1024),
    )(keys, values)
    return keys[None], values.reshape(1, length, heads, size)


def solution(mesh):
    in_specs = (
        P("ens", ("ctx", "group"), None),
        P("ens", ("ctx", "group"), None),
        P(),
        P("ens", "group", None),
        P("ens", "group", None),
    )
    out_specs = (P(("ens", "ctx"), "group", None, None), P(("ens", "ctx"), None, "group", None))
    return jax.shard_map(
        per_device, mesh=mesh, in_specs=in_specs, out_specs=out_specs, check_vma=False
    )
```
